32 devices in a mesh: pix: 32 (over z, y, x, core).
Axes of the slice: x: 2, y: 2, z: 4, core: 2. Of those that a mesh axis runs over, the one named last changes fastest.
Arguments:
- green: float32 [2048, 6144], P('pix'), may hold values from -200 to 200, as said below
- sketch: float32 [6144, 128], P('pix'), may hold values from -0.078125 to 0.078125
Outputs:
- basis: float32 [2048, 128], P('pix')
- projection: float32 [6144, 128], P('pix')
- spectrum_gram: float32 [128, 128], replicated
The draws below stay inside these ranges and needn't reach their ends.
Inputs may be any that keep to these rules, and one draw needn't show every extreme that they name: `green`: finite real entries; each patch's column has its own scale.
All inputs are finite; a program needn't handle non-finite values.
Results may differ from the reference program's by a relative error of at most 0.000086.
Values sent between devices are 32-bit elements; how exact they have to be, the bound alone decides.
A program may use at most 64 MiB of HBM per device.

```python
import jax
import jax.numpy as jnp
from jax import lax

PATCHES = 6144
RANK = 128
PIXELS = 2048


def draw_green(key, part):
    key_cols = jax.random.fold_in(key, 11)
    key_vals = jax.random.fold_in(key, 12)
    col_scale = jnp.exp(jax.random.uniform(key_cols, (1, PATCHES), jnp.float32, jnp.log(0.3), jnp.log(3.0)))
    values = jnp.clip(jax.random.normal(key_vals, (PIXELS, PATCHES), jnp.float32), -6.0, 6.0)
    return values * col_scale


def block_scale(stream_key, shape, pieces, least, largest):
    factor_of, own = 1.0, jax.random.fold_in(stream_key, 6)
    for dim, shards_of in pieces:
        steps = jnp.exp(jax.random.uniform(jax.random.fold_in(own, dim), (shards_of,), jnp.float32, least / len(pieces), largest / len(pieces)))
        factor_of = factor_of * jnp.repeat(steps, shape[dim] // shards_of).reshape([-1 if axis == dim else 1 for axis in range(len(shape))])
    return factor_of


def noise(stream_key, shape, spread, limit, shards=(), kind=jnp.bfloat16):
    values = spread * jax.random.normal(stream_key, shape, jnp.float32)
    if shards:
        values = values * block_scale(stream_key, shape, shards, -0.22, 0.18)
    return jnp.clip(values, -limit, limit).astype(kind)


def setup_inputs(seed: int = 0) -> dict:
    arg_keys = jax.random.split(jax.random.key(seed), 3)
    return {
        "green": draw_green(jax.random.fold_in(arg_keys[2], 71), 0),
        "sketch": noise(arg_keys[1], (PATCHES, RANK), PATCHES ** -0.5, 0.078125, ((0, 32),), jnp.float32),
    }


def reference(green, sketch):
    highest = lax.Precision.HIGHEST
    sketched = jnp.dot(green.astype(jnp.float32), sketch.astype(jnp.float32), precision=highest, preferred_element_type=jnp.float32)
    gram = jnp.dot(sketched.T.astype(jnp.float32), sketched.astype(jnp.float32), precision=highest, preferred_element_type=jnp.float32)
    lower = jnp.linalg.cholesky(gram)
    orthonormal = jax.scipy.linalg.solve_triangular(lower, sketched.T, lower=True).T
    basis = jnp.sqrt(jnp.float32(PIXELS)) * orthonormal
    projection = jnp.dot(green.T.astype(jnp.float32), orthonormal.astype(jnp.float32), precision=highest, preferred_element_type=jnp.float32)
    spectrum_gram = jnp.dot(projection.T.astype(jnp.float32), projection.astype(jnp.float32), precision=highest, preferred_element_type=jnp.float32) / jnp.float32(PATCHES)
    return (basis, projection, spectrum_gram)
```

```python
import functools

import jax
import jax.numpy as jnp
from jax import lax
from jax.experimental import pallas as pl
from jax.experimental.pallas import tpu as pltpu
from jax.sharding import PartitionSpec as P

MESH = pl.DeviceIdType.MESH
F32 = jnp.float32
BF16 = jnp.bfloat16
CHUNKS = 4


def grid_of(devices):
    cores = 2 if devices % 2 == 0 else 1
    chips = devices // cores
    side = 1
    for k in range(1, chips + 1):
        if chips % (k * k) == 0 and k * k * k <= chips:
            side = k
    return cores, side, side, chips // (side * side)


def split(v):
    hi = v.astype(BF16)
    return hi, (v - hi.astype(F32)).astype(BF16)


def dot(a, b, dims=((1,), (0,))):
    return lax.dot_general(a, b, (dims, ((), ())), preferred_element_type=F32)


def exact(a, b, dims=((1,), (0,))):
    return lax.dot_general(
        a, b, (dims, ((), ())), precision=lax.Precision.HIGHEST, preferred_element_type=F32
    )


def kernel(grid, total_pixels, patches, green, sketch, basis, projection, spectrum, scratch):
    C, X, Y, Z = grid
    assert C == 2
    r = scratch
    me = lax.axis_index("pix")
    c = lax.rem(me, C)
    x = lax.rem(me // C, X)
    y = lax.rem(me // (C * X), Y)
    z = me // (C * X * Y)
    rows = sketch.shape[0]
    rank = sketch.shape[1]
    pixels = green.shape[0]
    half_a = (rows // 2 + 7) // 8 * 8
    part_a, part_b = pl.ds(0, half_a), pl.ds(half_a, rows - half_a)
    slab = X * Y * C * rows

    def dev(zz, yy, xx, cc):
        return (((zz * Y + yy) * X + xx) * C + cc,)

    def at(v, d, n):
        return lax.rem(v + d + n, n)

    partner = dev(z, y, x, 1 - c)
    counter = [0]
    sends = []

    def copy(src, dst, recv, to):
        d = pltpu.make_async_remote_copy(
            src_ref=src, dst_ref=dst, send_sem=r["send"].at[counter[0]], recv_sem=recv,
            device_id=to, device_id_type=MESH,
        )
        counter[0] += 1
        sends.append(d)
        d.start()

    def arrive(dst, recv):
        pltpu.make_async_remote_copy(
            src_ref=dst, dst_ref=dst, send_sem=r["send"].at[0], recv_sem=recv,
            device_id=partner, device_id_type=MESH,
        ).wait_recv()

    barrier = pltpu.get_barrier_semaphore()
    plane = [(dy, dx) for dy in range(Y) for dx in range(X) if (dy, dx) != (0, 0)]
    peers = [partner]
    peers += [dev(z, at(y, dy, Y), at(x, dx, X), c) for dy, dx in plane]
    peers += [dev(at(z, d, Z), y, x, c) for d in range(1, Z)]
    for peer in peers:
        pl.semaphore_signal(barrier, inc=1, device_id=peer, device_id_type=MESH)
    pl.semaphore_wait(barrier, len(peers))

    near_first = sorted(range(1, Z), key=lambda d: min(d, Z - d))

    gat = r["gat"]
    slabs = [0] + near_first

    def ag1(s):
        zc = at(z, s, Z)
        if s == 0:
            mine_a, mine_b = sketch.at[part_a], sketch.at[part_b]
        else:
            arrive(gat.at[zc, y, x, c], r["agz"].at[s])
            mine_a, mine_b = gat.at[zc, y, x, c, part_a], gat.at[zc, y, x, c, part_b]
        for dx in range(1, X):
            copy(mine_a, gat.at[zc, y, x, c, part_a], r["agxa"].at[s, dx],
                 dev(z, y, at(x, dx, X), c))
        for dy in range(1, Y):
            copy(mine_b, gat.at[zc, y, x, c, part_b], r["agyb"].at[s, dy],
                 dev(z, at(y, dy, Y), x, c))
        if s == 0:
            for d in near_first:
                copy(sketch, gat.at[z, y, x, c], r["agz"].at[d], dev(at(z, -d, Z), y, x, c))
            gat[z, y, x, c] = sketch[...]

    def ag2(s):
        zc = at(z, s, Z)
        for dx in range(1, X):
            arrive(gat.at[zc, y, at(x, -dx, X), c, part_a], r["agxa"].at[s, dx])
        for dy in range(1, Y):
            ref = gat.at[zc, y, :, c, part_a]
            copy(ref, ref, r["agya"].at[s, dy], dev(z, at(y, dy, Y), x, c))
        for dy in range(1, Y):
            arrive(gat.at[zc, at(y, -dy, Y), x, c, part_b], r["agyb"].at[s, dy])
        for dx in range(1, X):
            ref = gat.at[zc, :, x, c, part_b]
            copy(ref, ref, r["agxb"].at[s, dx], dev(z, y, at(x, dx, X), c))

    def ag3(s):
        zc = at(z, s, Z)
        for dy in range(1, Y):
            arrive(gat.at[zc, at(y, -dy, Y), :, c, part_a], r["agya"].at[s, dy])
        for dx in range(1, X):
            arrive(gat.at[zc, :, at(x, -dx, X), c, part_b], r["agxb"].at[s, dx])
        ref = gat.at[zc, :, :, c]
        copy(ref, ref, r["agd"].at[s], partner)

    def ag4(s):
        zc = at(z, s, Z)
        arrive(gat.at[zc, :, :, 1 - c], r["agd"].at[s])
        block = gat[zc].reshape(slab, rank)
        g = green[:, pl.ds(pl.multiple_of(zc * slab, 128), slab)]
        g_hi, g_lo = split(g)
        b_hi, b_lo = split(block)
        both = dot(jnp.concatenate([g_hi, g_lo], axis=0), b_hi)
        out = both[:pixels] + both[pixels:] + dot(g_hi, b_lo)
        if s == 0:
            r["sketched"][...] = out
        else:
            r["sketched"][...] += out

    def pipeline(stages, items, extra=()):
        extra = list(extra)
        for t in range(len(items) + len(stages) - 1):
            for k, stage in enumerate(stages):
                if 0 <= t - k < len(items):
                    stage(items[t - k])
            if t > 0 and extra:
                extra.pop(0)()
        return extra

    pipeline([ag1, ag2, ag3, ag4], slabs)
    sketched = r["sketched"][...]
    s_hi, s_lo = split(sketched)
    packed = jnp.concatenate([s_hi, s_lo, s_hi, s_lo], axis=0)

    def all_sum(k, value, out):
        inc, mid, top = r["ar_in"].at[k], r["ar_mid"].at[k], r["ar_top"].at[k]
        h = rank // C
        keep = pl.ds(pl.multiple_of(c * h, h), h)
        give = pl.ds(pl.multiple_of((1 - c) * h, h), h)
        here = y * X + x

        def step0():
            r["ar_src"][k] = value()
            copy(r["ar_src"].at[k, give], inc, r["ar0"].at[k], partner)

        def step1():
            arrive(inc, r["ar0"].at[k])
            mid[here] = r["ar_src"][k, keep] + inc[...]
            for i, (dy, dx) in enumerate(plane):
                copy(mid.at[here], mid.at[here], r["ar1"].at[k, i],
                     dev(z, at(y, dy, Y), at(x, dx, X), c))

        def step2():
            for i, (dy, dx) in enumerate(plane):
                arrive(mid.at[at(y, -dy, Y) * X + at(x, -dx, X)], r["ar1"].at[k, i])
            top[z] = jnp.sum(mid[...], axis=0)
            for d in near_first:
                copy(top.at[z], top.at[z], r["ar2"].at[k, d], dev(at(z, d, Z), y, x, c))

        def step3():
            for d in near_first:
                arrive(top.at[at(z, -d, Z)], r["ar2"].at[k, d])
            out[keep, :] = jnp.sum(top[...], axis=0)
            copy(out.at[keep], out.at[keep], r["ar3"].at[k], partner)

        def step4():
            arrive(out.at[give], r["ar3"].at[k])

        return [step0, step1, step2, step3, step4]

    aug = r["aug"]
    lane = lax.broadcasted_iota(jnp.int32, (rank, rank), 1)
    row_of = lax.broadcasted_iota(jnp.int32, (rank, rank), 0)

    def eliminate(j, _):
        row = aug[pl.ds(j, 1), :]
        left = aug[:, :rank]
        col = jnp.sum(jnp.where(lane == j, left, 0.0), axis=1, keepdims=True)
        pivot = jnp.sum(jnp.where(lane[:1] == j, row[:, :rank], 0.0), axis=1, keepdims=True)
        f = jnp.where(row_of[:, :1] > j, col * (1.0 / pivot), 0.0)
        aug[...] = aug[...] - f * row
        return 0

    def chol(i):
        def run():
            if i == 0:
                aug[:, :rank] = r["gram"][...]
                aug[:, rank:] = jnp.where(lane == row_of, 1.0, 0.0)
            lax.fori_loop(rank // CHUNKS * i, rank // CHUNKS * (i + 1), eliminate, 0)

        return run

    part, q = r["part"], r["q"]

    def rs1(s):
        zo = at(z, s, Z)
        g_hi, g_lo = split(green[:, pl.ds(pl.multiple_of(zo * slab, 128), slab)])
        tall = jnp.concatenate([g_hi, g_hi, g_lo, g_lo], axis=0)
        part[s] = dot(tall, packed, ((0,), (0,))).reshape(Y, X, C, rows, rank)
        copy(part.at[s, :, :, 1 - c], r["rd"].at[s], r["rsd"].at[s], partner)

    def rs2(s):
        arrive(r["rd"].at[s], r["rsd"].at[s])
        q[s] = part[s, :, :, c] + r["rd"][s]
        for dy in range(1, Y):
            copy(q.at[s, at(y, dy, Y), :, part_a], r["rya"].at[s, dy], r["rsya"].at[s, dy],
                 dev(z, at(y, dy, Y), x, c))
        for dx in range(1, X):
            copy(q.at[s, :, at(x, dx, X), part_b], r["rxb"].at[s, dx], r["rsxb"].at[s, dx],
                 dev(z, y, at(x, dx, X), c))

    def rs3(s):
        total = q[s, y, :, part_a]
        for dy in range(1, Y):
            arrive(r["rya"].at[s, dy], r["rsya"].at[s, dy])
            total = total + r["rya"][s, dy]
        r["qa"][s] = total
        for dx in range(1, X):
            copy(r["qa"].at[s, at(x, dx, X)], r["rxa"].at[s, dx], r["rsxa"].at[s, dx],
                 dev(z, y, at(x, dx, X), c))
        total = q[s, :, x, part_b]
        for dx in range(1, X):
            arrive(r["rxb"].at[s, dx], r["rsxb"].at[s, dx])
            total = total + r["rxb"][s, dx]
        r["qb"][s] = total
        for dy in range(1, Y):
            copy(r["qb"].at[s, at(y, dy, Y)], r["ryb"].at[s, dy], r["rsyb"].at[s, dy],
                 dev(z, at(y, dy, Y), x, c))

    def rs4(s):
        total = r["qa"][s, x]
        for dx in range(1, X):
            arrive(r["rxa"].at[s, dx], r["rsxa"].at[s, dx])
            total = total + r["rxa"][s, dx]
        r["fin"][s, part_a] = total
        total = r["qb"][s, y]
        for dy in range(1, Y):
            arrive(r["ryb"].at[s, dy], r["rsyb"].at[s, dy])
            total = total + r["ryb"][s, dy]
        r["fin"][s, part_b] = total
        if s:
            copy(r["fin"].at[s], r["rz"].at[s], r["rsz"].at[s], dev(at(z, s, Z), y, x, c))

    gram_sum = all_sum(0, lambda: exact(sketched, sketched, ((0,), (0,))), r["gram"])
    gram_sum[0]()
    todo = gram_sum[1:] + [chol(i) for i in range(CHUNKS)]
    todo = pipeline([rs1, rs2, rs3, rs4], near_first[::-1] + [0], todo)

    raw = r["fin"][0]
    for s in range(1, Z):
        arrive(r["rz"].at[s], r["rsz"].at[s])
        raw = raw + r["rz"][s]
    spec_sum = all_sum(1, lambda: exact(raw, raw, ((0,), (0,))), r["spec"])
    for k, step in enumerate(spec_sum):
        step()
        if todo:
            todo.pop(0)()
    for job in todo:
        job()

    diag = jnp.sum(jnp.where(lane == row_of, aug[:, :rank], 0.0), axis=1, keepdims=True)
    inverse = aug[:, rank:] * lax.rsqrt(diag)
    basis[...] = jnp.sqrt(F32(total_pixels)) * exact(sketched, inverse, ((1,), (1,)))
    projection[...] = exact(raw, inverse, ((1,), (1,)))
    spectrum[...] = exact(exact(inverse, r["spec"][...]), inverse, ((1,), (1,))) / F32(patches)
    for d in sends:
        d.wait_send()


def body(grid, green, sketch):
    C, X, Y, Z = grid
    rows, rank = sketch.shape
    pixels, patches = green.shape
    half_a = (rows // 2 + 7) // 8 * 8
    half_b = rows - half_a
    plane = X * Y - 1

    def vmem(*shape):
        return pltpu.VMEM(shape, F32)

    def dma(*shape):
        return pltpu.SemaphoreType.DMA(shape)

    per_slab = 2 * (X - 1) + 2 * (Y - 1) + 1
    sends = 2 * (Z * per_slab + Z - 1) + 2 * (2 + plane + Z - 1)
    scratch = dict(
        gat=vmem(Z, Y, X, C, rows, rank), sketched=vmem(pixels, rank),
        part=vmem(Z, Y, X, C, rows, rank), rd=vmem(Z, Y, X, rows, rank),
        q=vmem(Z, Y, X, rows, rank),
        rya=vmem(Z, Y, X, half_a, rank), rxb=vmem(Z, X, Y, half_b, rank),
        qa=vmem(Z, X, half_a, rank), qb=vmem(Z, Y, half_b, rank),
        rxa=vmem(Z, X, half_a, rank), ryb=vmem(Z, Y, half_b, rank),
        fin=vmem(Z, rows, rank), rz=vmem(Z, rows, rank),
        ar_src=vmem(2, rank, rank), ar_in=vmem(2, rank // C, rank),
        ar_mid=vmem(2, X * Y, rank // C, rank), ar_top=vmem(2, Z, rank // C, rank),
        gram=vmem(rank, rank), spec=vmem(rank, rank), aug=vmem(rank, 2 * rank),
        send=dma(sends),
        agz=dma(Z), agxa=dma(Z, X), agyb=dma(Z, Y), agya=dma(Z, Y), agxb=dma(Z, X), agd=dma(Z),
        rsd=dma(Z), rsya=dma(Z, Y), rsxb=dma(Z, X), rsxa=dma(Z, X), rsyb=dma(Z, Y), rsz=dma(Z),
        ar0=dma(2), ar1=dma(2, plane), ar2=dma(2, Z), ar3=dma(2),
    )
    total_pixels = pixels * C * X * Y * Z
    return pl.pallas_call(
        functools.partial(kernel, grid, total_pixels, patches),
        out_shape=(
            jax.ShapeDtypeStruct((pixels, rank), F32),
            jax.ShapeDtypeStruct((rows, rank), F32),
            jax.ShapeDtypeStruct((rank, rank), F32),
        ),
        in_specs=[pl.BlockSpec(memory_space=pltpu.VMEM)] * 2,
        out_specs=(pl.BlockSpec(memory_space=pltpu.VMEM),) * 3,
        scratch_shapes=[scratch],
        compiler_params=pltpu.CompilerParams(
            collective_id=0, has_side_effects=True, vmem_limit_bytes=60 * 1024 * 1024
        ),
    )(green, sketch)


def solution(mesh):
    grid = grid_of(mesh.shape["pix"])
    in_specs = (P("pix", None), P("pix", None))
    out_specs = (P("pix", None), P("pix", None), P())
    return jax.shard_map(
        functools.partial(body, grid), mesh=mesh, in_specs=in_specs, out_specs=out_specs, check_vma=False
    )
```

```python
import functools

import jax
import jax.numpy as jnp
from jax import lax
from jax.experimental import pallas as pl
from jax.experimental.pallas import tpu as pltpu
from jax.sharding import PartitionSpec as P

MESH = pl.DeviceIdType.MESH
F32 = jnp.float32
BF16 = jnp.bfloat16


def grid_of(devices):
    cores = 2 if devices % 2 == 0 else 1
    chips = devices // cores
    side = 1
    for k in range(1, chips + 1):
        if chips % (k * k) == 0 and k * k * k <= chips:
            side = k
    return cores, side, side, chips // (side * side)


def split(v):
    hi = v.astype(BF16)
    return hi, (v - hi.astype(F32)).astype(BF16)


def dot(a, b, dims=((1,), (0,))):
    return lax.dot_general(a, b, (dims, ((), ())), preferred_element_type=F32)


def exact(a, b, dims=((1,), (0,))):
    return lax.dot_general(
        a, b, (dims, ((), ())), precision=lax.Precision.HIGHEST, preferred_element_type=F32
    )


def kernel(grid, total_pixels, green_in, sketch_in, basis, projection, inverse_out, spec, scratch):
    C, X, Y, Z = grid
    assert C == 2
    r = scratch
    me = lax.axis_index("pix")
    c = lax.rem(me, C)
    x = lax.rem(me // C, X)
    y = lax.rem(me // (C * X), Y)
    z = me // (C * X * Y)
    green, sketch = r["green"], r["sketch"]
    load_sketch = pltpu.make_async_copy(sketch_in, sketch, r["load"].at[0])
    load_green = pltpu.make_async_copy(green_in, green, r["load"].at[1])
    load_sketch.start()
    load_green.start()
    rows = sketch.shape[0]
    rank = sketch.shape[1]
    pixels = green.shape[0]
    half_a = (rows // 2 + 7) // 8 * 8
    part_a, part_b = pl.ds(0, half_a), pl.ds(half_a, rows - half_a)
    slab = X * Y * C * rows

    def dev(zz, yy, xx, cc):
        return (((zz * Y + yy) * X + xx) * C + cc,)

    def at(v, d, n):
        return lax.rem(v + d + n, n)

    partner = dev(z, y, x, 1 - c)
    counter = [0]
    sends = []

    def copy(src, dst, recv, to):
        d = pltpu.make_async_remote_copy(
            src_ref=src, dst_ref=dst, send_sem=r["send"].at[counter[0]], recv_sem=recv,
            device_id=to, device_id_type=MESH,
        )
        counter[0] += 1
        sends.append(d)
        d.start()

    def arrive(dst, recv):
        pltpu.make_async_remote_copy(
            src_ref=dst, dst_ref=dst, send_sem=r["send"].at[0], recv_sem=recv,
            device_id=partner, device_id_type=MESH,
        ).wait_recv()

    barrier = pltpu.get_barrier_semaphore()
    plane = [(dy, dx) for dy in range(Y) for dx in range(X) if (dy, dx) != (0, 0)]
    peers = [partner]
    peers += [dev(z, at(y, dy, Y), at(x, dx, X), c) for dy, dx in plane]
    peers += [dev(at(z, d, Z), y, x, c) for d in range(1, Z)]
    for peer in peers:
        pl.semaphore_signal(barrier, inc=1, device_id=peer, device_id_type=MESH)
    load_sketch.wait()
    pl.semaphore_wait(barrier, len(peers))

    short = jnp.minimum(z, Z - 1 - z)
    side = jnp.where(z <= Z - 1 - z, 1, -1)

    def near(p):
        sign = side if p % 2 else -side
        return z + jnp.where(p <= 2 * short, sign * ((p + 1) // 2), side * (p - short))

    others = range(1, Z)

    gat = r["gat"]

    def ag1(s):
        zc = near(s)
        if s == 0:
            mine_a, mine_b = sketch.at[part_a], sketch.at[part_b]
        else:
            arrive(gat.at[zc, y, x, c], r["agz"].at[zc])
            mine_a, mine_b = gat.at[zc, y, x, c, part_a], gat.at[zc, y, x, c, part_b]
        for dx in range(1, X):
            copy(mine_a, gat.at[zc, y, x, c, part_a], r["agxa"].at[s, dx],
                 dev(z, y, at(x, dx, X), c))
        for dy in range(1, Y):
            copy(mine_b, gat.at[zc, y, x, c, part_b], r["agyb"].at[s, dy],
                 dev(z, at(y, dy, Y), x, c))
        if s == 0:
            for p in others:
                copy(sketch, gat.at[z, y, x, c], r["agz"].at[z], dev(near(p), y, x, c))
            gat[z, y, x, c] = sketch[...]

    def ag2(s):
        zc = near(s)
        for dx in range(1, X):
            arrive(gat.at[zc, y, at(x, -dx, X), c, part_a], r["agxa"].at[s, dx])
        for dy in range(1, Y):
            ref = gat.at[zc, y, :, c, part_a]
            copy(ref, ref, r["agya"].at[s, dy], dev(z, at(y, dy, Y), x, c))
        for dy in range(1, Y):
            arrive(gat.at[zc, at(y, -dy, Y), x, c, part_b], r["agyb"].at[s, dy])
        for dx in range(1, X):
            ref = gat.at[zc, :, x, c, part_b]
            copy(ref, ref, r["agxb"].at[s, dx], dev(z, y, at(x, dx, X), c))

    def ag3(s):
        zc = near(s)
        for dy in range(1, Y):
            arrive(gat.at[zc, at(y, -dy, Y), :, c, part_a], r["agya"].at[s, dy])
        for dx in range(1, X):
            arrive(gat.at[zc, :, at(x, -dx, X), c, part_b], r["agxb"].at[s, dx])
        ref = gat.at[zc, :, :, c]
        copy(ref, ref, r["agd"].at[s], partner)

    def ag4(s):
        zc = near(s)
        arrive(gat.at[zc, :, :, 1 - c], r["agd"].at[s])
        if s == 0:
            load_green.wait()
        block = gat[zc].reshape(slab, rank)
        g = green[:, pl.ds(pl.multiple_of(zc * slab, 128), slab)]
        g_hi, g_lo = split(g)
        b_hi, b_lo = split(block)
        both = dot(jnp.concatenate([g_hi, g_lo], axis=0), b_hi)
        out = both[:pixels] + both[pixels:] + dot(g_hi, b_lo)
        if s == 0:
            r["sketched"][...] = out
        else:
            r["sketched"][...] += out

    def pipeline(stages, items, extra):
        for t in range(len(items) + len(stages) - 1):
            for k, stage in enumerate(stages):
                if 0 <= t - k < len(items):
                    stage(items[t - k])
            for job in extra.get(t, ()):
                job()

    pipeline([ag1, ag2, ag3, ag4], range(Z), {})
    sketched = r["sketched"][...]
    s_hi, s_lo = split(sketched)
    packed = jnp.concatenate([s_hi, s_lo, s_hi, s_lo], axis=0)

    def all_sum(k, value, out):
        inc, mid, top = r["ar_in"].at[k], r["ar_mid"].at[k], r["ar_top"].at[k]
        h = rank // C
        keep = pl.ds(pl.multiple_of(c * h, h), h)
        give = pl.ds(pl.multiple_of((1 - c) * h, h), h)
        here = y * X + x

        def step0():
            r["ar_src"][k] = value()
            copy(r["ar_src"].at[k, give], inc, r["ar0"].at[k], partner)

        def step1():
            arrive(inc, r["ar0"].at[k])
            mid[here] = r["ar_src"][k, keep] + inc[...]
            for i, (dy, dx) in enumerate(plane):
                copy(mid.at[here], mid.at[here], r["ar1"].at[k, i],
                     dev(z, at(y, dy, Y), at(x, dx, X), c))

        def step2():
            for i, (dy, dx) in enumerate(plane):
                arrive(mid.at[at(y, -dy, Y) * X + at(x, -dx, X)], r["ar1"].at[k, i])
            top[z] = jnp.sum(mid[...], axis=0)
            for p in others:
                copy(top.at[z], top.at[z], r["ar2"].at[k, z], dev(near(p), y, x, c))

        def step3():
            for p in others:
                arrive(top.at[near(p)], r["ar2"].at[k, near(p)])
            out[keep, :] = jnp.sum(top[...], axis=0)
            copy(out.at[keep], out.at[keep], r["ar3"].at[k], partner)

        def step4():
            arrive(out.at[give], r["ar3"].at[k])

        return [step0, step1, step2, step3, step4]

    aug = r["aug"]
    lane = lax.broadcasted_iota(jnp.int32, (rank, rank), 1)
    row_of = lax.broadcasted_iota(jnp.int32, (rank, rank), 0)

    def eliminate(j, _):
        row = aug[pl.ds(j, 1), :]
        left = aug[:, :rank]
        col = jnp.sum(jnp.where(lane == j, left, 0.0), axis=1, keepdims=True)
        pivot = jnp.sum(jnp.where(lane[:1] == j, row[:, :rank], 0.0), axis=1, keepdims=True)
        f = jnp.where(row_of[:, :1] > j, col * (1.0 / pivot), 0.0)
        aug[...] = aug[...] - f * row
        return 0

    def begin():
        aug[:, :rank] = r["gram"][...]
        aug[:, rank:] = jnp.where(lane == row_of, 1.0, 0.0)

    def chol(first, last):
        def run():
            lax.fori_loop(first, last, eliminate, 0)

        return run

    def finish():
        diag = jnp.sum(jnp.where(lane == row_of, aug[:, :rank], 0.0), axis=1, keepdims=True)
        inverse = aug[:, rank:] * lax.rsqrt(diag)
        inverse_out[...] = inverse
        basis[...] = jnp.sqrt(F32(total_pixels)) * exact(sketched, inverse, ((1,), (1,)))
        projection[...] = exact(raw, inverse, ((1,), (1,)))

    part, q = r["part"], r["q"]

    def rs1(s):
        zo = near(s)
        g_hi, g_lo = split(green[:, pl.ds(pl.multiple_of(zo * slab, 128), slab)])
        tall = jnp.concatenate([g_hi, g_hi, g_lo, g_lo], axis=0)
        part[s] = dot(tall, packed, ((0,), (0,))).reshape(Y, X, C, rows, rank)
        copy(part.at[s, :, :, 1 - c], r["rd"].at[s], r["rsd"].at[s], partner)

    def rs2(s):
        arrive(r["rd"].at[s], r["rsd"].at[s])
        q[s] = part[s, :, :, c] + r["rd"][s]
        for dy in range(1, Y):
            copy(q.at[s, at(y, dy, Y), :, part_a], r["rya"].at[s, dy], r["rsya"].at[s, dy],
                 dev(z, at(y, dy, Y), x, c))
        for dx in range(1, X):
            copy(q.at[s, :, at(x, dx, X), part_b], r["rxb"].at[s, dx], r["rsxb"].at[s, dx],
                 dev(z, y, at(x, dx, X), c))

    def rs3(s):
        total = q[s, y, :, part_a]
        for dy in range(1, Y):
            arrive(r["rya"].at[s, dy], r["rsya"].at[s, dy])
            total = total + r["rya"][s, dy]
        r["qa"][s] = total
        for dx in range(1, X):
            copy(r["qa"].at[s, at(x, dx, X)], r["rxa"].at[s, dx], r["rsxa"].at[s, dx],
                 dev(z, y, at(x, dx, X), c))
        total = q[s, :, x, part_b]
        for dx in range(1, X):
            arrive(r["rxb"].at[s, dx], r["rsxb"].at[s, dx])
            total = total + r["rxb"][s, dx]
        r["qb"][s] = total
        for dy in range(1, Y):
            copy(r["qb"].at[s, at(y, dy, Y)], r["ryb"].at[s, dy], r["rsyb"].at[s, dy],
                 dev(z, at(y, dy, Y), x, c))

    def rs4(s):
        total = r["qa"][s, x]
        for dx in range(1, X):
            arrive(r["rxa"].at[s, dx], r["rsxa"].at[s, dx])
            total = total + r["rxa"][s, dx]
        r["fin"][s, part_a] = total
        total = r["qb"][s, y]
        for dy in range(1, Y):
            arrive(r["ryb"].at[s, dy], r["rsyb"].at[s, dy])
            total = total + r["ryb"][s, dy]
        r["fin"][s, part_b] = total
        if s:
            copy(r["fin"].at[s], r["rz"].at[z], r["rsz"].at[z], dev(near(s), y, x, c))

    def cut(k):
        return rank * k // 16

    gram_sum = all_sum(0, lambda: exact(sketched, sketched, ((0,), (0,))), r["gram"])
    gram_sum[0]()
    last = Z + 2
    extra = {1: gram_sum[1:2], last - 3: gram_sum[2:3], last - 1: gram_sum[3:4],
             last: gram_sum[4:5] + [begin, chol(0, cut(2))]}
    pipeline([rs1, rs2, rs3, rs4], range(Z)[::-1], extra)

    raw = r["fin"][0]
    for p in others:
        arrive(r["rz"].at[near(p)], r["rsz"].at[near(p)])
        raw = raw + r["rz"][near(p)]
    spec_sum = all_sum(1, lambda: exact(raw, raw, ((0,), (0,))), spec)
    spec_sum[0]()
    chol(cut(2), cut(4))()
    spec_sum[1]()
    chol(cut(4), cut(9))()
    spec_sum[2]()
    chol(cut(9), cut(16))()
    spec_sum[3]()
    finish()
    spec_sum[4]()
    for d in sends:
        d.wait_send()


def finish_kernel(patches, basis_in, projection_in, inverse_in, spec_in, basis, projection, spectrum):
    inverse = inverse_in[...]
    basis[...] = basis_in[...]
    projection[...] = projection_in[...]
    spectrum[...] = exact(exact(inverse, spec_in[...]), inverse, ((1,), (1,))) / F32(patches)


def body(grid, green, sketch):
    C, X, Y, Z = grid
    rows, rank = sketch.shape
    pixels, patches = green.shape
    half_a = (rows // 2 + 7) // 8 * 8
    half_b = rows - half_a
    plane = X * Y - 1

    def vmem(*shape):
        return pltpu.VMEM(shape, F32)

    def dma(*shape):
        return pltpu.SemaphoreType.DMA(shape)

    per_slab = 2 * (X - 1) + 2 * (Y - 1) + 1
    sends = 2 * (Z * per_slab + Z - 1) + 2 * (2 + plane + Z - 1)
    scratch = dict(
        gat=vmem(Z, Y, X, C, rows, rank), sketched=vmem(pixels, rank),
        part=vmem(Z, Y, X, C, rows, rank), rd=vmem(Z, Y, X, rows, rank),
        q=vmem(Z, Y, X, rows, rank),
        rya=vmem(Z, Y, X, half_a, rank), rxb=vmem(Z, X, Y, half_b, rank),
        qa=vmem(Z, X, half_a, rank), qb=vmem(Z, Y, half_b, rank),
        rxa=vmem(Z, X, half_a, rank), ryb=vmem(Z, Y, half_b, rank),
        fin=vmem(Z, rows, rank), rz=vmem(Z, rows, rank),
        ar_src=vmem(2, rank, rank), ar_in=vmem(2, rank // C, rank),
        ar_mid=vmem(2, X * Y, rank // C, rank), ar_top=vmem(2, Z, rank // C, rank),
        gram=vmem(rank, rank), green=vmem(pixels, patches), sketch=vmem(rows, rank), aug=vmem(rank, 2 * rank),
        send=dma(sends), load=dma(2),
        agz=dma(Z), agxa=dma(Z, X), agyb=dma(Z, Y), agya=dma(Z, Y), agxb=dma(Z, X), agd=dma(Z),
        rsd=dma(Z), rsya=dma(Z, Y), rsxb=dma(Z, X), rsxa=dma(Z, X), rsyb=dma(Z, Y), rsz=dma(Z),
        ar0=dma(2), ar1=dma(2, plane), ar2=dma(2, Z), ar3=dma(2),
    )
    total_pixels = pixels * C * X * Y * Z
    tall = jax.ShapeDtypeStruct((pixels, rank), F32)
    wide = jax.ShapeDtypeStruct((rows, rank), F32)
    square = jax.ShapeDtypeStruct((rank, rank), F32)
    whole = pl.BlockSpec(memory_space=pltpu.VMEM)
    parts = pl.pallas_call(
        functools.partial(kernel, grid, total_pixels),
        out_shape=(tall, wide, square, square),
        in_specs=[pl.BlockSpec(memory_space=pl.ANY)] * 2,
        out_specs=(whole,) * 4,
        scratch_shapes=[scratch],
        compiler_params=pltpu.CompilerParams(
            collective_id=0, has_side_effects=True, vmem_limit_bytes=63 * 1024 * 1024
        ),
    )(green, sketch)
    return pl.pallas_call(
        functools.partial(finish_kernel, patches),
        out_shape=(tall, wide, square),
        in_specs=[whole] * 4,
        out_specs=(whole,) * 3,
    )(*parts)


def solution(mesh):
    grid = grid_of(mesh.shape["pix"])
    in_specs = (P("pix", None), P("pix", None))
    out_specs = (P("pix", None), P("pix", None), P())
    return jax.shard_map(
        functools.partial(body, grid), mesh=mesh, in_specs=in_specs, out_specs=out_specs, check_vma=False
    )
```

```python
import functools

import jax
import jax.numpy as jnp
from jax import lax
from jax.experimental import pallas as pl
from jax.experimental.pallas import tpu as pltpu
from jax.sharding import PartitionSpec as P

MESH = pl.DeviceIdType.MESH
F32 = jnp.float32
BF16 = jnp.bfloat16
PANEL = 8


def grid_of(devices):
    cores = 2 if devices % 2 == 0 else 1
    chips = devices // cores
    side = 1
    for k in range(1, chips + 1):
        if chips % (k * k) == 0 and k * k * k <= chips:
            side = k
    return cores, side, side, chips // (side * side)


def split(v):
    hi = v.astype(BF16)
    return hi, (v - hi.astype(F32)).astype(BF16)


def thirds(v):
    a = v.astype(BF16).astype(F32)
    b = (v - a).astype(BF16).astype(F32)
    return a, b, v - a - b


def dot(a, b, dims=((1,), (0,))):
    return lax.dot_general(a, b, (dims, ((), ())), preferred_element_type=F32)


def exact(a, b, dims=((1,), (0,))):
    return lax.dot_general(
        a, b, (dims, ((), ())), precision=lax.Precision.HIGHEST, preferred_element_type=F32
    )


def kernel(grid, total_pixels, green_in, sketch_in, basis, projection, inverse_out, spec, scratch):
    C, X, Y, Z = grid
    assert C == 2
    r = scratch
    me = lax.axis_index("pix")
    c = lax.rem(me, C)
    x = lax.rem(me // C, X)
    y = lax.rem(me // (C * X), Y)
    z = me // (C * X * Y)
    green, sketch = r["green"], r["sketch"]
    load_sketch = pltpu.make_async_copy(sketch_in, sketch, r["load"].at[0])
    load_green = pltpu.make_async_copy(green_in, green, r["load"].at[1])
    load_sketch.start()
    load_green.start()
    rows = sketch.shape[0]
    rank = sketch.shape[1]
    pixels = green.shape[0]
    half_a = (rows // 2 + 7) // 8 * 8
    part_a, part_b = pl.ds(0, half_a), pl.ds(half_a, rows - half_a)
    slab = X * Y * C * rows

    def dev(zz, yy, xx, cc):
        return (((zz * Y + yy) * X + xx) * C + cc,)

    def at(v, d, n):
        return lax.rem(v + d + n, n)

    partner = dev(z, y, x, 1 - c)
    counter = [0]
    sends = []

    def copy(src, dst, recv, to):
        d = pltpu.make_async_remote_copy(
            src_ref=src, dst_ref=dst, send_sem=r["send"].at[counter[0]], recv_sem=recv,
            device_id=to, device_id_type=MESH,
        )
        counter[0] += 1
        sends.append(d)
        d.start()

    def arrive(dst, recv):
        pltpu.make_async_remote_copy(
            src_ref=dst, dst_ref=dst, send_sem=r["send"].at[0], recv_sem=recv,
            device_id=partner, device_id_type=MESH,
        ).wait_recv()

    barrier = pltpu.get_barrier_semaphore()
    plane = [(dy, dx) for dy in range(Y) for dx in range(X) if (dy, dx) != (0, 0)]
    peers = [partner]
    peers += [dev(z, at(y, dy, Y), at(x, dx, X), c) for dy, dx in plane]
    peers += [dev(at(z, d, Z), y, x, c) for d in range(1, Z)]
    for peer in peers:
        pl.semaphore_signal(barrier, inc=1, device_id=peer, device_id_type=MESH)
    load_sketch.wait()
    pl.semaphore_wait(barrier, len(peers))

    short = jnp.minimum(z, Z - 1 - z)
    side = jnp.where(z <= Z - 1 - z, 1, -1)

    def near(p):
        sign = side if p % 2 else -side
        return z + jnp.where(p <= 2 * short, sign * ((p + 1) // 2), side * (p - short))

    others = range(1, Z)

    gat = r["gat"]

    def ag1(s):
        zc = near(s)
        if s == 0:
            mine_a, mine_b = sketch.at[part_a], sketch.at[part_b]
        else:
            arrive(gat.at[zc, y, x, c], r["agz"].at[zc])
            mine_a, mine_b = gat.at[zc, y, x, c, part_a], gat.at[zc, y, x, c, part_b]
        for dx in range(1, X):
            copy(mine_a, gat.at[zc, y, x, c, part_a], r["agxa"].at[s, dx],
                 dev(z, y, at(x, dx, X), c))
        for dy in range(1, Y):
            copy(mine_b, gat.at[zc, y, x, c, part_b], r["agyb"].at[s, dy],
                 dev(z, at(y, dy, Y), x, c))
        if s == 0:
            for p in others:
                copy(sketch, gat.at[z, y, x, c], r["agz"].at[z], dev(near(p), y, x, c))
            gat[z, y, x, c] = sketch[...]

    def ag2(s):
        zc = near(s)
        for dx in range(1, X):
            arrive(gat.at[zc, y, at(x, -dx, X), c, part_a], r["agxa"].at[s, dx])
        for dy in range(1, Y):
            ref = gat.at[zc, y, :, c, part_a]
            copy(ref, ref, r["agya"].at[s, dy], dev(z, at(y, dy, Y), x, c))
        for dy in range(1, Y):
            arrive(gat.at[zc, at(y, -dy, Y), x, c, part_b], r["agyb"].at[s, dy])
        for dx in range(1, X):
            ref = gat.at[zc, :, x, c, part_b]
            copy(ref, ref, r["agxb"].at[s, dx], dev(z, y, at(x, dx, X), c))

    def ag3(s):
        zc = near(s)
        for dy in range(1, Y):
            arrive(gat.at[zc, at(y, -dy, Y), :, c, part_a], r["agya"].at[s, dy])
        for dx in range(1, X):
            arrive(gat.at[zc, :, at(x, -dx, X), c, part_b], r["agxb"].at[s, dx])
        ref = gat.at[zc, :, :, c]
        copy(ref, ref, r["agd"].at[s], partner)

    def ag4(s):
        zc = near(s)
        arrive(gat.at[zc, :, :, 1 - c], r["agd"].at[s])
        if s == 0:
            load_green.wait()
        block = gat[zc].reshape(slab, rank)
        g = green[:, pl.ds(pl.multiple_of(zc * slab, 128), slab)]
        g_hi, g_lo = split(g)
        b_hi, b_lo = split(block)
        both = dot(jnp.concatenate([g_hi, g_lo], axis=0), b_hi)
        out = both[:pixels] + both[pixels:] + dot(g_hi, b_lo)
        if s == 0:
            r["sketched"][...] = out
        else:
            r["sketched"][...] += out

    def pipeline(stages, items, extra):
        for t in range(len(items) + len(stages) - 1):
            for k, stage in enumerate(stages):
                if 0 <= t - k < len(items):
                    stage(items[t - k])
            for job in extra.get(t, ()):
                job()

    pipeline([ag1, ag2, ag3, ag4], range(Z), {})
    sketched = r["sketched"][...]
    s_hi, s_lo = split(sketched)
    packed = jnp.concatenate([s_hi, s_lo, s_hi, s_lo], axis=0)

    def spread_sum(k, value):
        here = y * X + x
        q = rank // (C * X * Y)
        src, inc, red, mid, top, res = (r[n].at[k] for n in ("s_src", "s_in", "s_red", "s_mid", "s_top", "s_res"))

        def step0():
            v = value()
            for i in range(C):
                for w in range(X * Y):
                    first = (i * X * Y + w) * q
                    src[i, w] = v[first : first + q]
            copy(src.at[1 - c], inc, r["sp0"].at[k], partner)

        def step1():
            arrive(inc, r["sp0"].at[k])
            red[...] = src[c] + inc[...]
            mid[here] = red[here]
            for i, (dy, dx) in enumerate(plane):
                yy, xx = at(y, dy, Y), at(x, dx, X)
                copy(red.at[yy * X + xx], mid.at[here], r["sp1"].at[k, i], dev(z, yy, xx, c))

        def step2():
            for i, (dy, dx) in enumerate(plane):
                arrive(mid.at[at(y, -dy, Y) * X + at(x, -dx, X)], r["sp1"].at[k, i])
            top[z] = jnp.sum(mid[...], axis=0)
            for p in others:
                copy(top.at[z], top.at[z], r["sp2"].at[k, z], dev(near(p), y, x, c))

        def step3():
            for p in others:
                arrive(top.at[near(p)], r["sp2"].at[k, near(p)])
            res[c, here] = jnp.sum(top[...], axis=0)
            for i, (dy, dx) in enumerate(plane):
                copy(res.at[c, here], res.at[c, here], r["sp3"].at[k, i],
                     dev(z, at(y, dy, Y), at(x, dx, X), c))

        def step4():
            for i, (dy, dx) in enumerate(plane):
                arrive(res.at[c, at(y, -dy, Y) * X + at(x, -dx, X)], r["sp3"].at[k, i])
            copy(res.at[c], res.at[c], r["sp4"].at[k], partner)

        def step5():
            arrive(res.at[1 - c], r["sp4"].at[k])

        def total():
            return jnp.concatenate([res[i, w] for i in range(C) for w in range(X * Y)], axis=0)

        return [step0, step1, step2, step3, step4, step5], total

    aug = r["aug"]
    lane = lax.broadcasted_iota(jnp.int32, (rank, rank), 1)
    row_of = lax.broadcasted_iota(jnp.int32, (rank, rank), 0)

    def eliminate(p, _):
        first = pl.multiple_of(p * PANEL, PANEL)
        lanes = lane[:PANEL]
        index = row_of[:PANEL, :1]
        block = aug[pl.ds(first, PANEL), :]
        left = block[:, :rank]
        cols = [
            jnp.sum(jnp.where(lanes == first + k, left, 0.0), axis=1, keepdims=True)
            for k in range(PANEL)
        ]
        scale = jnp.zeros((PANEL, 1), F32)
        for k in range(PANEL):
            inv = 1.0 / cols[k][k : k + 1]
            f = jnp.where(index > k, cols[k] * inv, 0.0)
            for m in range(k + 1, PANEL):
                cols[m] = cols[m] - f * cols[m][k : k + 1]
            block = block - f * block[k : k + 1]
            scale = jnp.where(index == k, inv, scale)
        u = thirds(jnp.where(lanes >= first + PANEL, block[:, :rank] * scale, 0.0))
        v = thirds(block)
        lhs = jnp.concatenate([u[i] for i in (0, 0, 0, 1, 1, 2)], axis=0).astype(BF16)
        rhs = jnp.concatenate([v[i] for i in (0, 1, 2, 0, 1, 0)], axis=0).astype(BF16)
        aug[...] = aug[...] - dot(lhs, rhs, ((0,), (0,)))
        aug[pl.ds(first, PANEL), :] = block
        return 0

    def begin():
        aug[:, :rank] = gram_total()
        aug[:, rank:] = jnp.where(lane == row_of, 1.0, 0.0)

    def chol(first, last):
        lax.fori_loop(first, last, eliminate, 0)

    def finish():
        diag = jnp.sum(jnp.where(lane == row_of, aug[:, :rank], 0.0), axis=1, keepdims=True)
        inverse = aug[:, rank:] * lax.rsqrt(diag)
        inverse_out[...] = inverse
        basis[...] = jnp.sqrt(F32(total_pixels)) * exact(sketched, inverse, ((1,), (1,)))
        projection[...] = exact(raw, inverse, ((1,), (1,)))

    part, q = r["part"], r["q"]

    def rs1(s):
        zo = near(s)
        g_hi, g_lo = split(green[:, pl.ds(pl.multiple_of(zo * slab, 128), slab)])
        tall = jnp.concatenate([g_hi, g_hi, g_lo, g_lo], axis=0)
        part[s] = dot(tall, packed, ((0,), (0,))).reshape(Y, X, C, rows, rank)
        copy(part.at[s, :, :, 1 - c], r["rd"].at[s], r["rsd"].at[s], partner)

    def rs2(s):
        arrive(r["rd"].at[s], r["rsd"].at[s])
        q[s] = part[s, :, :, c] + r["rd"][s]
        for dy in range(1, Y):
            copy(q.at[s, at(y, dy, Y), :, part_a], r["rya"].at[s, dy], r["rsya"].at[s, dy],
                 dev(z, at(y, dy, Y), x, c))
        for dx in range(1, X):
            copy(q.at[s, :, at(x, dx, X), part_b], r["rxb"].at[s, dx], r["rsxb"].at[s, dx],
                 dev(z, y, at(x, dx, X), c))

    def rs3(s):
        total = q[s, y, :, part_a]
        for dy in range(1, Y):
            arrive(r["rya"].at[s, dy], r["rsya"].at[s, dy])
            total = total + r["rya"][s, dy]
        r["qa"][s] = total
        for dx in range(1, X):
            copy(r["qa"].at[s, at(x, dx, X)], r["rxa"].at[s, dx], r["rsxa"].at[s, dx],
                 dev(z, y, at(x, dx, X), c))
        total = q[s, :, x, part_b]
        for dx in range(1, X):
            arrive(r["rxb"].at[s, dx], r["rsxb"].at[s, dx])
            total = total + r["rxb"][s, dx]
        r["qb"][s] = total
        for dy in range(1, Y):
            copy(r["qb"].at[s, at(y, dy, Y)], r["ryb"].at[s, dy], r["rsyb"].at[s, dy],
                 dev(z, at(y, dy, Y), x, c))

    def rs4(s):
        total = r["qa"][s, x]
        for dx in range(1, X):
            arrive(r["rxa"].at[s, dx], r["rsxa"].at[s, dx])
            total = total + r["rxa"][s, dx]
        r["fin"][s, part_a] = total
        total = r["qb"][s, y]
        for dy in range(1, Y):
            arrive(r["ryb"].at[s, dy], r["rsyb"].at[s, dy])
            total = total + r["ryb"][s, dy]
        r["fin"][s, part_b] = total
        if s:
            copy(r["fin"].at[s], r["rz"].at[z], r["rsz"].at[z], dev(near(s), y, x, c))

    gram, gram_total = spread_sum(0, lambda: exact(sketched, sketched, ((0,), (0,))))
    last = Z + 2
    extra = {0: gram[:1], 1: gram[1:2], last - 3: gram[2:3], last - 1: gram[3:4], last: gram[4:5]}
    pipeline([rs1, rs2, rs3, rs4], range(Z)[::-1], extra)

    raw = r["fin"][0]
    for p in others:
        arrive(r["rz"].at[near(p)], r["rsz"].at[near(p)])
        raw = raw + r["rz"][near(p)]
    spec_sum, spec_total = spread_sum(1, lambda: exact(raw, raw, ((0,), (0,))))
    panels = rank // PANEL
    spec_sum[0]()
    gram[5]()
    begin()
    spec_sum[1]()
    chol(0, panels * 2 // 5)
    spec_sum[2]()
    chol(panels * 2 // 5, panels * 4 // 5)
    spec_sum[3]()
    chol(panels * 4 // 5, panels)
    finish()
    spec_sum[4]()
    spec_sum[5]()
    spec[...] = spec_total()
    for d in sends:
        d.wait_send()


def finish_kernel(patches, basis_in, projection_in, inverse_in, spec_in, basis, projection, spectrum):
    inverse = inverse_in[...]
    basis[...] = basis_in[...]
    projection[...] = projection_in[...]
    spectrum[...] = exact(exact(inverse, spec_in[...]), inverse, ((1,), (1,))) / F32(patches)


def body(grid, green, sketch):
    C, X, Y, Z = grid
    rows, rank = sketch.shape
    pixels, patches = green.shape
    half_a = (rows // 2 + 7) // 8 * 8
    half_b = rows - half_a
    plane = X * Y - 1
    few = rank // (C * X * Y)

    def vmem(*shape):
        return pltpu.VMEM(shape, F32)

    def dma(*shape):
        return pltpu.SemaphoreType.DMA(shape)

    per_slab = 2 * (X - 1) + 2 * (Y - 1) + 1
    sends = 2 * (Z * per_slab + Z - 1) + 2 * (2 + 2 * plane + Z - 1)
    scratch = dict(
        gat=vmem(Z, Y, X, C, rows, rank), sketched=vmem(pixels, rank),
        part=vmem(Z, Y, X, C, rows, rank), rd=vmem(Z, Y, X, rows, rank),
        q=vmem(Z, Y, X, rows, rank),
        rya=vmem(Z, Y, X, half_a, rank), rxb=vmem(Z, X, Y, half_b, rank),
        qa=vmem(Z, X, half_a, rank), qb=vmem(Z, Y, half_b, rank),
        rxa=vmem(Z, X, half_a, rank), ryb=vmem(Z, Y, half_b, rank),
        fin=vmem(Z, rows, rank), rz=vmem(Z, rows, rank),
        s_src=vmem(2, C, X * Y, few, rank), s_in=vmem(2, X * Y, few, rank),
        s_red=vmem(2, X * Y, few, rank), s_mid=vmem(2, X * Y, few, rank),
        s_top=vmem(2, Z, few, rank), s_res=vmem(2, C, X * Y, few, rank),
        green=vmem(pixels, patches), sketch=vmem(rows, rank), aug=vmem(rank, 2 * rank),
        send=dma(sends), load=dma(2),
        agz=dma(Z), agxa=dma(Z, X), agyb=dma(Z, Y), agya=dma(Z, Y), agxb=dma(Z, X), agd=dma(Z),
        rsd=dma(Z), rsya=dma(Z, Y), rsxb=dma(Z, X), rsxa=dma(Z, X), rsyb=dma(Z, Y), rsz=dma(Z),
        sp0=dma(2), sp1=dma(2, plane), sp2=dma(2, Z), sp3=dma(2, plane), sp4=dma(2),
    )
    total_pixels = pixels * C * X * Y * Z
    tall = jax.ShapeDtypeStruct((pixels, rank), F32)
    wide = jax.ShapeDtypeStruct((rows, rank), F32)
    square = jax.ShapeDtypeStruct((rank, rank), F32)
    whole = pl.BlockSpec(memory_space=pltpu.VMEM)
    parts = pl.pallas_call(
        functools.partial(kernel, grid, total_pixels),
        out_shape=(tall, wide, square, square),
        in_specs=[pl.BlockSpec(memory_space=pl.ANY)] * 2,
        out_specs=(whole,) * 4,
        scratch_shapes=[scratch],
        compiler_params=pltpu.CompilerParams(
            collective_id=0, has_side_effects=True, vmem_limit_bytes=63 * 1024 * 1024
        ),
    )(green, sketch)
    return pl.pallas_call(
        functools.partial(finish_kernel, patches),
        out_shape=(tall, wide, square),
        in_specs=[whole] * 4,
        out_specs=(whole,) * 3,
    )(*parts)


def solution(mesh):
    grid = grid_of(mesh.shape["pix"])
    in_specs = (P("pix", None), P("pix", None))
    out_specs = (P("pix", None), P("pix", None), P())
    return jax.shard_map(
        functools.partial(body, grid), mesh=mesh, in_specs=in_specs, out_specs=out_specs, check_vma=False
    )
```

```python
import functools

import jax
import jax.numpy as jnp
from jax import lax
from jax.experimental import pallas as pl
from jax.experimental.pallas import tpu as pltpu
from jax.sharding import PartitionSpec as P

MESH = pl.DeviceIdType.MESH
F32 = jnp.float32
BF16 = jnp.bfloat16
PANEL = 8


def grid_of(devices):
    cores = 2 if devices % 2 == 0 else 1
    chips = devices // cores
    side = 1
    for k in range(1, chips + 1):
        if chips % (k * k) == 0 and k * k * k <= chips:
            side = k
    return cores, side, side, chips // (side * side)


def split(v):
    hi = v.astype(BF16)
    return hi, (v - hi.astype(F32)).astype(BF16)


def thirds(v):
    a = v.astype(BF16).astype(F32)
    b = (v - a).astype(BF16).astype(F32)
    return a, b, v - a - b


def dot(a, b, dims=((1,), (0,))):
    return lax.dot_general(a, b, (dims, ((), ())), preferred_element_type=F32)


def exact(a, b, dims=((1,), (0,))):
    return lax.dot_general(
        a, b, (dims, ((), ())), precision=lax.Precision.HIGHEST, preferred_element_type=F32
    )


def kernel(grid, total_pixels, green_in, sketch_in, basis, projection, inverse_out, spec, scratch):
    C, X, Y, Z = grid
    assert C == 2
    r = scratch
    me = lax.axis_index("pix")
    c = lax.rem(me, C)
    x = lax.rem(me // C, X)
    y = lax.rem(me // (C * X), Y)
    z = me // (C * X * Y)
    green, sketch = r["green"], r["sketch"]
    load_sketch = pltpu.make_async_copy(sketch_in, sketch, r["load"].at[0])
    load_green = pltpu.make_async_copy(green_in, green, r["load"].at[1])
    load_sketch.start()
    load_green.start()
    rows = sketch.shape[0]
    rank = sketch.shape[1]
    pixels = green.shape[0]
    half_a = (rows // 2 + 7) // 8 * 8
    part_a, part_b = pl.ds(0, half_a), pl.ds(half_a, rows - half_a)
    slab = X * Y * C * rows

    def dev(zz, yy, xx, cc):
        return (((zz * Y + yy) * X + xx) * C + cc,)

    def at(v, d, n):
        return lax.rem(v + d + n, n)

    partner = dev(z, y, x, 1 - c)
    counter = [0]
    sends = []

    def copy(src, dst, recv, to):
        d = pltpu.make_async_remote_copy(
            src_ref=src, dst_ref=dst, send_sem=r["send"].at[counter[0]], recv_sem=recv,
            device_id=to, device_id_type=MESH,
        )
        counter[0] += 1
        sends.append(d)
        d.start()

    def arrive(dst, recv):
        pltpu.make_async_remote_copy(
            src_ref=dst, dst_ref=dst, send_sem=r["send"].at[0], recv_sem=recv,
            device_id=partner, device_id_type=MESH,
        ).wait_recv()

    barrier = pltpu.get_barrier_semaphore()
    plane = [(dy, dx) for dy in range(Y) for dx in range(X) if (dy, dx) != (0, 0)]
    peers = [partner]
    peers += [dev(z, at(y, dy, Y), at(x, dx, X), c) for dy, dx in plane]
    peers += [dev(at(z, d, Z), y, x, c) for d in range(1, Z)]
    for peer in peers:
        pl.semaphore_signal(barrier, inc=1, device_id=peer, device_id_type=MESH)
    load_sketch.wait()
    pl.semaphore_wait(barrier, len(peers))

    short = jnp.minimum(z, Z - 1 - z)
    side = jnp.where(z <= Z - 1 - z, 1, -1)

    def near(p):
        sign = side if p % 2 else -side
        return z + jnp.where(p <= 2 * short, sign * ((p + 1) // 2), side * (p - short))

    others = range(1, Z)

    gat = r["gat"]

    def ag1(s):
        zc = near(s)
        if s == 0:
            mine_a, mine_b = sketch.at[part_a], sketch.at[part_b]
        else:
            arrive(gat.at[zc, y, x, c], r["agz"].at[zc])
            mine_a, mine_b = gat.at[zc, y, x, c, part_a], gat.at[zc, y, x, c, part_b]
        for dx in range(1, X):
            copy(mine_a, gat.at[zc, y, x, c, part_a], r["agxa"].at[s, dx],
                 dev(z, y, at(x, dx, X), c))
        for dy in range(1, Y):
            copy(mine_b, gat.at[zc, y, x, c, part_b], r["agyb"].at[s, dy],
                 dev(z, at(y, dy, Y), x, c))
        if s == 0:
            for p in others:
                copy(sketch, gat.at[z, y, x, c], r["agz"].at[z], dev(near(p), y, x, c))
            gat[z, y, x, c] = sketch[...]

    def ag2(s):
        zc = near(s)
        for dx in range(1, X):
            arrive(gat.at[zc, y, at(x, -dx, X), c, part_a], r["agxa"].at[s, dx])
        for dy in range(1, Y):
            ref = gat.at[zc, y, :, c, part_a]
            copy(ref, ref, r["agya"].at[s, dy], dev(z, at(y, dy, Y), x, c))
        for dy in range(1, Y):
            arrive(gat.at[zc, at(y, -dy, Y), x, c, part_b], r["agyb"].at[s, dy])
        for dx in range(1, X):
            ref = gat.at[zc, :, x, c, part_b]
            copy(ref, ref, r["agxb"].at[s, dx], dev(z, y, at(x, dx, X), c))

    def ag3(s):
        zc = near(s)
        for dy in range(1, Y):
            arrive(gat.at[zc, at(y, -dy, Y), :, c, part_a], r["agya"].at[s, dy])
        for dx in range(1, X):
            arrive(gat.at[zc, :, at(x, -dx, X), c, part_b], r["agxb"].at[s, dx])
        ref = gat.at[zc, :, :, c]
        copy(ref, ref, r["agd"].at[s], partner)

    def ag4(s):
        zc = near(s)
        arrive(gat.at[zc, :, :, 1 - c], r["agd"].at[s])
        if s == 0:
            load_green.wait()
        block = gat[zc].reshape(slab, rank)
        g = green[:, pl.ds(pl.multiple_of(zc * slab, 128), slab)]
        g_hi, g_lo = split(g)
        b_hi, b_lo = split(block)
        both = dot(jnp.concatenate([g_hi, g_lo], axis=0), b_hi)
        out = both[:pixels] + both[pixels:] + dot(g_hi, b_lo)
        if s == 0:
            r["sketched"][...] = out
        else:
            r["sketched"][...] += out

    def pipeline(stages, items, extra):
        for t in range(len(items) + len(stages) - 1):
            for k, stage in enumerate(stages):
                if 0 <= t - k < len(items):
                    stage(items[t - k])
            for job in extra.get(t, ()):
                job()

    pipeline([ag1, ag2, ag3, ag4], range(Z), {})
    sketched = r["sketched"][...]
    s_hi, s_lo = split(sketched)
    packed = jnp.concatenate([s_hi, s_lo, s_hi, s_lo], axis=0)

    def all_sum(k, value, out):
        inc, mid, top = r["ar_in"].at[k], r["ar_mid"].at[k], r["ar_top"].at[k]
        h = rank // C
        keep = pl.ds(pl.multiple_of(c * h, h), h)
        give = pl.ds(pl.multiple_of((1 - c) * h, h), h)
        here = y * X + x

        def step0():
            r["ar_src"][k] = value()
            copy(r["ar_src"].at[k, give], inc, r["ar0"].at[k], partner)

        def step1():
            arrive(inc, r["ar0"].at[k])
            mid[here] = r["ar_src"][k, keep] + inc[...]
            for i, (dy, dx) in enumerate(plane):
                copy(mid.at[here], mid.at[here], r["ar1"].at[k, i],
                     dev(z, at(y, dy, Y), at(x, dx, X), c))

        def step2():
            for i, (dy, dx) in enumerate(plane):
                arrive(mid.at[at(y, -dy, Y) * X + at(x, -dx, X)], r["ar1"].at[k, i])
            top[z] = jnp.sum(mid[...], axis=0)
            for p in others:
                copy(top.at[z], top.at[z], r["ar2"].at[k, z], dev(near(p), y, x, c))

        def step3():
            for p in others:
                arrive(top.at[near(p)], r["ar2"].at[k, near(p)])
            out[keep, :] = jnp.sum(top[...], axis=0)
            copy(out.at[keep], out.at[keep], r["ar3"].at[k], partner)

        def step4():
            arrive(out.at[give], r["ar3"].at[k])

        return [step0, step1, step2, step3, step4]

    def spread_sum(k, value):
        here = y * X + x
        q = rank // (C * X * Y)
        src, inc, red, mid, top, res = (r[n].at[k] for n in ("s_src", "s_in", "s_red", "s_mid", "s_top", "s_res"))

        def step0():
            v = value()
            for i in range(C):
                for w in range(X * Y):
                    first = (i * X * Y + w) * q
                    src[i, w] = v[first : first + q]
            copy(src.at[1 - c], inc, r["sp0"].at[k], partner)

        def step1():
            arrive(inc, r["sp0"].at[k])
            red[...] = src[c] + inc[...]
            mid[here] = red[here]
            for i, (dy, dx) in enumerate(plane):
                yy, xx = at(y, dy, Y), at(x, dx, X)
                copy(red.at[yy * X + xx], mid.at[here], r["sp1"].at[k, i], dev(z, yy, xx, c))

        def step2():
            for i, (dy, dx) in enumerate(plane):
                arrive(mid.at[at(y, -dy, Y) * X + at(x, -dx, X)], r["sp1"].at[k, i])
            top[z] = jnp.sum(mid[...], axis=0)
            for p in others:
                copy(top.at[z], top.at[z], r["sp2"].at[k, z], dev(near(p), y, x, c))

        def step3():
            for p in others:
                arrive(top.at[near(p)], r["sp2"].at[k, near(p)])
            res[c, here] = jnp.sum(top[...], axis=0)
            for i, (dy, dx) in enumerate(plane):
                copy(res.at[c, here], res.at[c, here], r["sp3"].at[k, i],
                     dev(z, at(y, dy, Y), at(x, dx, X), c))

        def step4():
            for i, (dy, dx) in enumerate(plane):
                arrive(res.at[c, at(y, -dy, Y) * X + at(x, -dx, X)], r["sp3"].at[k, i])
            copy(res.at[c], res.at[c], r["sp4"].at[k], partner)

        def step5():
            arrive(res.at[1 - c], r["sp4"].at[k])

        def total():
            return jnp.concatenate([res[i, w] for i in range(C) for w in range(X * Y)], axis=0)

        return [step0, step1, step2, step3, step4, step5], total

    aug = r["aug"]
    lane = lax.broadcasted_iota(jnp.int32, (rank, rank), 1)
    row_of = lax.broadcasted_iota(jnp.int32, (rank, rank), 0)

    def eliminate(p, _):
        first = pl.multiple_of(p * PANEL, PANEL)
        lanes = lane[:PANEL]
        index = row_of[:PANEL, :1]
        block = aug[pl.ds(first, PANEL), :]
        left = block[:, :rank]
        cols = [
            jnp.sum(jnp.where(lanes == first + k, left, 0.0), axis=1, keepdims=True)
            for k in range(PANEL)
        ]
        scale = jnp.zeros((PANEL, 1), F32)
        for k in range(PANEL):
            inv = 1.0 / cols[k][k : k + 1]
            f = jnp.where(index > k, cols[k] * inv, 0.0)
            for m in range(k + 1, PANEL):
                cols[m] = cols[m] - f * cols[m][k : k + 1]
            block = block - f * block[k : k + 1]
            scale = jnp.where(index == k, inv, scale)
        u = thirds(jnp.where(lanes >= first + PANEL, block[:, :rank] * scale, 0.0))
        v = thirds(block)
        lhs = jnp.concatenate([u[i] for i in (0, 0, 0, 1, 1, 2)], axis=0).astype(BF16)
        rhs = jnp.concatenate([v[i] for i in (0, 1, 2, 0, 1, 0)], axis=0).astype(BF16)
        aug[...] = aug[...] - dot(lhs, rhs, ((0,), (0,)))
        aug[pl.ds(first, PANEL), :] = block
        return 0

    def begin():
        aug[:, :rank] = gram_total()
        aug[:, rank:] = jnp.where(lane == row_of, 1.0, 0.0)

    def chol(first, last):
        lax.fori_loop(first, last, eliminate, 0)

    def finish():
        diag = jnp.sum(jnp.where(lane == row_of, aug[:, :rank], 0.0), axis=1, keepdims=True)
        inverse = aug[:, rank:] * lax.rsqrt(diag)
        inverse_out[...] = inverse
        basis[...] = jnp.sqrt(F32(total_pixels)) * exact(sketched, inverse, ((1,), (1,)))
        projection[...] = exact(raw, inverse, ((1,), (1,)))

    part, q = r["part"], r["q"]

    def rs1(s):
        zo = near(s)
        g_hi, g_lo = split(green[:, pl.ds(pl.multiple_of(zo * slab, 128), slab)])
        tall = jnp.concatenate([g_hi, g_hi, g_lo, g_lo], axis=0)
        part[s] = dot(tall, packed, ((0,), (0,))).reshape(Y, X, C, rows, rank)
        copy(part.at[s, :, :, 1 - c], r["rd"].at[s], r["rsd"].at[s], partner)

    def rs2(s):
        arrive(r["rd"].at[s], r["rsd"].at[s])
        q[s] = part[s, :, :, c] + r["rd"][s]
        for dy in range(1, Y):
            copy(q.at[s, at(y, dy, Y), :, part_a], r["rya"].at[s, dy], r["rsya"].at[s, dy],
                 dev(z, at(y, dy, Y), x, c))
        for dx in range(1, X):
            copy(q.at[s, :, at(x, dx, X), part_b], r["rxb"].at[s, dx], r["rsxb"].at[s, dx],
                 dev(z, y, at(x, dx, X), c))

    def rs3(s):
        total = q[s, y, :, part_a]
        for dy in range(1, Y):
            arrive(r["rya"].at[s, dy], r["rsya"].at[s, dy])
            total = total + r["rya"][s, dy]
        r["qa"][s] = total
        for dx in range(1, X):
            copy(r["qa"].at[s, at(x, dx, X)], r["rxa"].at[s, dx], r["rsxa"].at[s, dx],
                 dev(z, y, at(x, dx, X), c))
        total = q[s, :, x, part_b]
        for dx in range(1, X):
            arrive(r["rxb"].at[s, dx], r["rsxb"].at[s, dx])
            total = total + r["rxb"][s, dx]
        r["qb"][s] = total
        for dy in range(1, Y):
            copy(r["qb"].at[s, at(y, dy, Y)], r["ryb"].at[s, dy], r["rsyb"].at[s, dy],
                 dev(z, at(y, dy, Y), x, c))

    def rs4(s):
        total = r["qa"][s, x]
        for dx in range(1, X):
            arrive(r["rxa"].at[s, dx], r["rsxa"].at[s, dx])
            total = total + r["rxa"][s, dx]
        r["fin"][s, part_a] = total
        total = r["qb"][s, y]
        for dy in range(1, Y):
            arrive(r["ryb"].at[s, dy], r["rsyb"].at[s, dy])
            total = total + r["ryb"][s, dy]
        r["fin"][s, part_b] = total
        if s:
            copy(r["fin"].at[s], r["rz"].at[z], r["rsz"].at[z], dev(near(s), y, x, c))

    gram, gram_total = spread_sum(0, lambda: exact(sketched, sketched, ((0,), (0,))))
    last = Z + 2
    extra = {0: gram[:1], 1: gram[1:2], last - 3: gram[2:3], last - 1: gram[3:4], last: gram[4:5]}
    pipeline([rs1, rs2, rs3, rs4], range(Z)[::-1], extra)

    raw = r["fin"][0]
    for p in others:
        arrive(r["rz"].at[near(p)], r["rsz"].at[near(p)])
        raw = raw + r["rz"][near(p)]
    spec_sum = all_sum(0, lambda: exact(raw, raw, ((0,), (0,))), spec)
    panels = rank // PANEL
    spec_sum[0]()
    gram[5]()
    begin()
    spec_sum[1]()
    chol(0, panels * 2 // 5)
    spec_sum[2]()
    chol(panels * 2 // 5, panels)
    spec_sum[3]()
    finish()
    spec_sum[4]()
    for d in sends:
        d.wait_send()


def finish_kernel(patches, basis_in, projection_in, inverse_in, spec_in, basis, projection, spectrum):
    inverse = inverse_in[...]
    basis[...] = basis_in[...]
    projection[...] = projection_in[...]
    spectrum[...] = exact(exact(inverse, spec_in[...]), inverse, ((1,), (1,))) / F32(patches)


def body(grid, green, sketch):
    C, X, Y, Z = grid
    rows, rank = sketch.shape
    pixels, patches = green.shape
    half_a = (rows // 2 + 7) // 8 * 8
    half_b = rows - half_a
    plane = X * Y - 1
    few = rank // (C * X * Y)

    def vmem(*shape):
        return pltpu.VMEM(shape, F32)

    def dma(*shape):
        return pltpu.SemaphoreType.DMA(shape)

    per_slab = 2 * (X - 1) + 2 * (Y - 1) + 1
    sends = 2 * (Z * per_slab + Z - 1) + 2 * (2 + 2 * plane + Z - 1)
    scratch = dict(
        gat=vmem(Z, Y, X, C, rows, rank), sketched=vmem(pixels, rank),
        part=vmem(Z, Y, X, C, rows, rank), rd=vmem(Z, Y, X, rows, rank),
        q=vmem(Z, Y, X, rows, rank),
        rya=vmem(Z, Y, X, half_a, rank), rxb=vmem(Z, X, Y, half_b, rank),
        qa=vmem(Z, X, half_a, rank), qb=vmem(Z, Y, half_b, rank),
        rxa=vmem(Z, X, half_a, rank), ryb=vmem(Z, Y, half_b, rank),
        fin=vmem(Z, rows, rank), rz=vmem(Z, rows, rank),
        ar_src=vmem(1, rank, rank), ar_in=vmem(1, rank // C, rank),
        ar_mid=vmem(1, X * Y, rank // C, rank), ar_top=vmem(1, Z, rank // C, rank),
        s_src=vmem(2, C, X * Y, few, rank), s_in=vmem(2, X * Y, few, rank),
        s_red=vmem(2, X * Y, few, rank), s_mid=vmem(2, X * Y, few, rank),
        s_top=vmem(2, Z, few, rank), s_res=vmem(2, C, X * Y, few, rank),
        green=vmem(pixels, patches), sketch=vmem(rows, rank), aug=vmem(rank, 2 * rank),
        send=dma(sends), load=dma(2),
        agz=dma(Z), agxa=dma(Z, X), agyb=dma(Z, Y), agya=dma(Z, Y), agxb=dma(Z, X), agd=dma(Z),
        rsd=dma(Z), rsya=dma(Z, Y), rsxb=dma(Z, X), rsxa=dma(Z, X), rsyb=dma(Z, Y), rsz=dma(Z),
        ar0=dma(1), ar1=dma(1, plane), ar2=dma(1, Z), ar3=dma(1),
        sp0=dma(2), sp1=dma(2, plane), sp2=dma(2, Z), sp3=dma(2, plane), sp4=dma(2),
    )
    total_pixels = pixels * C * X * Y * Z
    tall = jax.ShapeDtypeStruct((pixels, rank), F32)
    wide = jax.ShapeDtypeStruct((rows, rank), F32)
    square = jax.ShapeDtypeStruct((rank, rank), F32)
    whole = pl.BlockSpec(memory_space=pltpu.VMEM)
    parts = pl.pallas_call(
        functools.partial(kernel, grid, total_pixels),
        out_shape=(tall, wide, square, square),
        in_specs=[pl.BlockSpec(memory_space=pl.ANY)] * 2,
        out_specs=(whole,) * 4,
        scratch_shapes=[scratch],
        compiler_params=pltpu.CompilerParams(
            collective_id=0, has_side_effects=True, vmem_limit_bytes=63 * 1024 * 1024
        ),
    )(green, sketch)
    return pl.pallas_call(
        functools.partial(finish_kernel, patches),
        out_shape=(tall, wide, square),
        in_specs=[whole] * 4,
        out_specs=(whole,) * 3,
    )(*parts)


def solution(mesh):
    grid = grid_of(mesh.shape["pix"])
    in_specs = (P("pix", None), P("pix", None))
    out_specs = (P("pix", None), P("pix", None), P())
    return jax.shard_map(
        functools.partial(body, grid), mesh=mesh, in_specs=in_specs, out_specs=out_specs, check_vma=False
    )
```
